32 devices in a mesh: dp: 2 (over z, core), tp: 16 (over x, y).
Axes of the slice: x: 4, y: 4, z: 1, core: 2. Of those that a mesh axis runs over, the one named last changes fastest.
The devices are a block of a 4x4x8 slice.
Arguments:
- x: bfloat16 [4096, 2048], P('dp'), parts along dimension 0
- dy: bfloat16 [4096, 2048], P('dp'), parts along dimension 0
- gate: bfloat16 [4096, 8192], P('dp', 'tp'), parts along dimension 0
- up: bfloat16 [4096, 8192], P('dp', 'tp'), parts along dimension 0
- w_gate: bfloat16 [2048, 8192], P(None, 'tp')
- w_up: bfloat16 [2048, 8192], P(None, 'tp')
- w_down: bfloat16 [8192, 2048], P('tp')
Outputs:
- output 1: bfloat16 [4096, 2048], P('dp'), parts along dimension 0
- output 2: bfloat16 [4096, 8192], P('dp', 'tp'), parts along dimension 0
- output 3: bfloat16 [4096, 8192], P('dp', 'tp'), parts along dimension 0
- output 4: bfloat16 [16384, 2048], P(('dp', 'tp')), parts along dimension 0
There are 2 independent parts. The reference program is written for one: setup_inputs(seed, part) draws one part's arguments, and reference() takes and returns one part's arrays. A program takes and returns all parts, laid end to end along the dimension named above; an argument that names none is the same for every part.
All inputs are finite; a program needn't handle non-finite values.
Results may differ from the reference program's by a relative error of at most 0.012.
Values are sent between devices in bfloat16 or wider.
A program may use at most 768 MiB of HBM per device.

```python
import jax
import jax.numpy as jnp

ROWS = 2048
D = 2048
FF = 8192


def act(gate, up):
    return jax.nn.silu(gate) * up


def setup_inputs(seed: int = 0, part: int = 0) -> dict:
    kx, ky, ka, kb, kg, ku, kd = jax.random.split(jax.random.key(seed), 7)
    kx, ky, ka, kb = (jax.random.fold_in(k, part) for k in (kx, ky, ka, kb))
    drawn = {
        "x": jax.random.normal(kx, (ROWS, D), jnp.float32),
        "dy": jax.random.normal(ky, (ROWS, D), jnp.float32),
        "gate": jax.random.normal(ka, (ROWS, FF), jnp.float32),
        "up": jax.random.normal(kb, (ROWS, FF), jnp.float32),
        "w_gate": jax.random.normal(kg, (D, FF), jnp.float32) * D**-0.5,
        "w_up": jax.random.normal(ku, (D, FF), jnp.float32) * D**-0.5,
        "w_down": jax.random.normal(kd, (FF, D), jnp.float32) * FF**-0.5,
    }
    return {k: v.astype(jnp.bfloat16) for k, v in drawn.items()}


def reference(x, dy, gate, up, w_gate, w_up, w_down):
    hidden, back = jax.vjp(act, gate.astype(jnp.float32), up.astype(jnp.float32))
    d_hidden = jnp.dot(dy, w_down.T, preferred_element_type=jnp.float32)
    d_gate, d_up = (g.astype(jnp.bfloat16) for g in back(d_hidden))
    dx = jnp.dot(d_gate, w_gate.T, preferred_element_type=jnp.float32) + jnp.dot(d_up, w_up.T, preferred_element_type=jnp.float32)
    dw_gate = jnp.dot(x.T, d_gate, preferred_element_type=jnp.float32)
    dw_up = jnp.dot(x.T, d_up, preferred_element_type=jnp.float32)
    dw_down = jnp.dot(hidden.astype(jnp.bfloat16).T, dy, preferred_element_type=jnp.float32)
    return tuple(g.astype(jnp.bfloat16) for g in (dx, dw_gate, dw_up, dw_down))
```

```python
import functools
import math

import jax
import jax.numpy as jnp
from jax import lax
from jax.experimental import pallas as pl
from jax.experimental.pallas import tpu as pltpu
from jax.sharding import PartitionSpec as P

SIDE = 4
CHUNKS = 4
A, B, C, A2, B2, C2, G20, G21, R2, G10, G11, R1 = range(12)
NT = (((1,), (1,)), ((), ()))
NN = (((1,), (0,)), ((), ()))


def dot(a, b, dims):
    return lax.dot_general(a, b, dims, preferred_element_type=jnp.float32)


def chunk_rows(rows):
    return [rows // CHUNKS] * CHUNKS


def body(chunks, x, dy, gate, up, w_gate, w_up, w_down, dx, dw_gate, dw_up, dw_down,
         wd, wgu, dgu, hid_t, dyb, gb, ub, xb, xt, st_a, st_b, r_a, r_b, r_c, c_term, own,
         s2_a, s2_b, r2_a, r2_b, r2_c, lsem, ssem, rsem):
    d = x.shape[1]
    ff = gate.shape[1]
    nb = d // (2 * SIDE)
    starts = [sum(chunks[:k]) for k in range(len(chunks))]
    t = lax.axis_index("tp")
    px, py = lax.div(t, SIDE), lax.rem(t, SIDE)

    def to(axis, s):
        step = 1 + (SIDE - 2) * s
        return lax.rem(px + (1 - axis) * step, SIDE) * SIDE + lax.rem(py + axis * step, SIDE)

    def on(axis):
        return px * (1 - axis) + py * axis

    def local(src, dst, i):
        return pltpu.make_async_copy(src, dst, lsem.at[i])

    def send(kind, k, i, src, dst, axis):
        s = lax.rem(i, 2)
        return pltpu.make_async_remote_copy(
            src_ref=src, dst_ref=dst, send_sem=ssem.at[kind, k, i], recv_sem=rsem.at[kind, k, i],
            device_id={"tp": to(axis, s)}, device_id_type=pl.DeviceIdType.MESH,
        )

    def loop(n, f):
        lax.fori_loop(0, n, lambda i, c: (f(i), c)[1], 0)

    nk = len(chunks)
    load_wd = local(w_down, wd, 0)
    load_wg = local(w_gate, wgu.at[:, pl.ds(0, ff)], 1)
    load_wu = local(w_up, wgu.at[:, pl.ds(ff, ff)], 2)

    def load_dy(k):
        rows = pl.ds(starts[k], chunks[k])
        return local(dy.at[rows], dyb.at[rows], 3 + k)

    def load_gu(k):
        rows, slot = pl.ds(starts[k], chunks[k]), pl.ds(0, chunks[k])
        return (local(gate.at[rows], gb.at[k % 2, slot], 3 + nk + k),
                local(up.at[rows], ub.at[k % 2, slot], 3 + 2 * nk + k))

    def load_x(j, slot):
        return local(x.at[:, pl.ds(pl.multiple_of(j * nb, nb), nb)], xb.at[slot], 3 + 3 * nk + slot)

    load_wd.start()
    load_dy(0).start()
    for c in load_gu(0):
        c.start()
    load_wg.start()
    load_wu.start()
    if nk > 1:
        load_dy(1).start()
        for c in load_gu(1):
            c.start()
    for k in range(2, nk):
        load_dy(k).start()
    load_x(0, 0).start()
    load_x(1, 1).start()

    barrier = pltpu.get_barrier_semaphore()
    for axis in range(2):
        for s in range(2):
            pl.semaphore_signal(barrier, inc=1, device_id={"tp": to(axis, s)}, device_id_type=pl.DeviceIdType.MESH)

    def ru(k):
        return chunks[k] // 2

    def rs(k):
        return chunks[k] // (2 * SIDE)

    def unit_rows(k, u):
        return pl.ds(starts[k] + u * ru(k), ru(k))

    def u1(k):
        return pl.ds(starts[k] // 2, ru(k))

    def u2(k):
        return pl.ds(starts[k] // (2 * SIDE), rs(k))

    def term(k, u, h, j):
        w = pl.ds(pl.multiple_of((h * SIDE + j) * nb, nb), nb)
        return dot(dgu[unit_rows(k, u), :], wgu[w, :], NT)

    def sub(k, q):
        return pl.ds(pl.multiple_of(starts[k] // 2 + q * rs(k), 16), rs(k))

    def region(k, u, h, j, q=None):
        cols = pl.ds(pl.multiple_of((h * SIDE + j) * nb, nb), nb)
        if q is None:
            return dx.at[pl.ds(pl.multiple_of(starts[k] + u * ru(k), 16), ru(k)), cols]
        return dx.at[pl.ds(pl.multiple_of(starts[k] + u * ru(k) + q * rs(k), 16), rs(k)), cols]

    def mod(v):
        return lax.rem(v, SIDE)

    def m_a(k, i, h):
        return send(A, k, i, st_a.at[i, u1(k)], r_a.at[i, u1(k)], h)

    def m_b(k, i, h):
        return send(B, k, i, st_b.at[i, u1(k)], r_b.at[i, u1(k)], h)

    def m_c(k, i, h):
        return send(C, k, i, r_a.at[i, u1(k)], r_c.at[i, u1(k)], h)

    def m_a2(k, i, h):
        return send(A2, k, i, s2_a.at[i, u2(k)], r2_a.at[i, u2(k)], 1 - h)

    def m_b2(k, i, h):
        return send(B2, k, i, s2_b.at[i, u2(k)], r2_b.at[i, u2(k)], 1 - h)

    def m_c2(k, i, h):
        return send(C2, k, i, r2_a.at[i, u2(k)], r2_c.at[i, u2(k)], 1 - h)

    def m_g2(k, i, h, s, n):
        u = s if n == 0 else 1 - s
        where = region(k, u, h, on(h), on(1 - h))
        return send(G20 + n, k, i, where, where, 1 - h)

    def m_r2(k, i, h, s):
        where = region(k, s, h, on(h), mod(on(1 - h) + SIDE - 1 + 2 * s))
        return send(R2, k, i, where, where, 1 - h)

    def m_g1(k, i, h, s, n):
        u = s if n == 0 else 1 - s
        where = region(k, u, h, on(h))
        return send(G10 + n, k, i, where, where, h)

    def m_r1(k, i, h, s):
        where = region(k, s, h, mod(on(h) + SIDE - 1 + 2 * s))
        return send(R1, k, i, where, where, h)

    def hs(i):
        return lax.div(i, 2), lax.rem(i, 2)

    def bf(v):
        return v.astype(jnp.bfloat16)

    def f32(v):
        return v.astype(jnp.float32)

    def stage_hidden(k):
        sm = min(256, chunks[k])
        nn = min(256, ff)
        load_dy(k).wait()
        for c in load_gu(k):
            c.wait()
        if k == 0:
            load_wd.wait()

        def tile(m):
            rows = pl.ds(pl.multiple_of(starts[k] + m * sm, sm), sm)
            part = pl.ds(pl.multiple_of(m * sm, sm), sm)
            for n in range(ff // nn):
                cols = pl.ds(n * nn, nn)
                dh = dot(dyb[rows, :], wd[cols, :], NT)
                g, v = f32(gb[k % 2, part, cols]), f32(ub[k % 2, part, cols])
                sg = 1.0 / (1.0 + jnp.exp(-g))
                silu = g * sg
                dgu[rows, cols] = bf(dh * v * (sg + silu * (1.0 - sg)))
                dgu[rows, pl.ds(ff + n * nn, nn)] = bf(dh * silu)
                hid_t[cols, rows] = bf(silu * v).T

        loop(chunks[k] // sm, tile)
        if k + 2 < nk:
            for c in load_gu(k + 2):
                c.start()

    def stage_a(k):
        if k == 0:
            load_wg.wait()
            load_wu.wait()

        def half(h):
            for s in range(2):
                st_a[2 * h + s, u1(k), :] = bf(term(k, s, h, mod(on(h) + 2)))
            if k == 0:
                pl.when(h == 0)(lambda: pl.semaphore_wait(barrier, 4))
            for s in range(2):
                m_a(k, 2 * h + s, h).start()

        loop(2, half)

    def stage_b(k):
        def each(i):
            h, s = hs(i)
            j = mod(on(h) + 1 + 2 * s)
            st_b[i, u1(k), :] = bf(term(k, 1 - s, h, j))
            m_b(k, i, h).start()
            c_term[i, u1(k), :] = term(k, s, h, j)

        loop(4, each)

    def stage_c(k):
        def each(i):
            h, s = hs(i)
            m_a(k, i, h).wait_recv()
            r_a[i, u1(k), :] = bf(c_term[i, u1(k), :] + f32(r_a[i, u1(k), :]))
            m_c(k, i, h).start()

        loop(4, each)

    def stage_own(k):
        def each(h):
            for u in range(2):
                own[h, u, u1(k), :] = term(k, u, h, on(h))

        loop(2, each)

    def stage_o(k):
        def each(h):
            for i in range(2):
                m_b(k, 2 * h + i, h).wait_recv()
                m_c(k, 2 * h + i, h).wait_recv()
            for u in range(2):
                own[h, u, u1(k), :] += f32(r_c[2 * h + u, u1(k), :]) + f32(r_b[2 * h + 1 - u, u1(k), :])
            q = on(1 - h)
            for s in range(2):
                s2_a[2 * h + s, u2(k), :] = bf(own[h, s, sub(k, mod(q + 2)), :])
                m_a2(k, 2 * h + s, h).start()
            for s in range(2):
                s2_b[2 * h + s, u2(k), :] = bf(own[h, 1 - s, sub(k, mod(q + 1 + 2 * s)), :])
                m_b2(k, 2 * h + s, h).start()

        loop(2, each)

    def stage_c2(k):
        def each(i):
            h, s = hs(i)
            m_a2(k, i, h).wait_recv()
            r2_a[i, u2(k), :] = bf(own[h, s, sub(k, mod(on(1 - h) + 1 + 2 * s)), :] + f32(r2_a[i, u2(k), :]))
            m_c2(k, i, h).start()

        loop(4, each)

    def stage_o2(k):
        def each(h):
            for i in range(2):
                m_b2(k, 2 * h + i, h).wait_recv()
                m_c2(k, 2 * h + i, h).wait_recv()
            q = on(1 - h)
            for u in range(2):
                total = own[h, u, sub(k, q), :] + f32(r2_c[2 * h + u, u2(k), :]) + f32(r2_b[2 * h + 1 - u, u2(k), :])
                region(k, u, h, on(h), q)[...] = bf(total)
            for n in range(2):
                for s in range(2):
                    m_g2(k, 2 * h + s, h, s, n).start()

        loop(2, each)

    def stage_r2(k):
        def each(h):
            for s in range(2):
                m_g2(k, 2 * h + s, h, s, 0).wait_recv()
                m_r2(k, 2 * h + s, h, s).start()

        loop(2, each)

    def stage_g1(k):
        def each(h):
            for s in range(2):
                m_g2(k, 2 * h + s, h, s, 1).wait_recv()
                m_r2(k, 2 * h + s, h, s).wait_recv()
            for n in range(2):
                for s in range(2):
                    m_g1(k, 2 * h + s, h, s, n).start()

        loop(2, each)

    def stage_r1(k):
        def each(h):
            for s in range(2):
                m_g1(k, 2 * h + s, h, s, 0).wait_recv()
                m_r1(k, 2 * h + s, h, s).start()

        loop(2, each)

    def stage_end(k):
        def each(h):
            for s in range(2):
                i = 2 * h + s
                m_g1(k, i, h, s, 1).wait_recv()
                m_r1(k, i, h, s).wait_recv()

        loop(2, each)

    def sent(k):
        def each(h):
            for s in range(2):
                i = 2 * h + s
                for m in (m_a, m_b, m_c, m_a2, m_b2, m_c2):
                    m(k, i, h).wait_send()
                for n in range(2):
                    m_g2(k, i, h, s, n).wait_send()
                    m_g1(k, i, h, s, n).wait_send()
                m_r2(k, i, h, s).wait_send()
                m_r1(k, i, h, s).wait_send()

        loop(2, each)

    tiles = d // nb

    def tile_gu(j):
        slot = lax.rem(j, 2)
        load_x(j, slot).wait()
        xt[...] = xb[slot].T
        pl.when(j + 2 < tiles)(lambda: load_x(j + 2, slot).start())
        nn = min(256, ff)
        rows = pl.ds(pl.multiple_of(j * nb, nb), nb)

        def cols_of(n):
            cols = pl.ds(pl.multiple_of(n * nn, nn), nn)
            dw_gate[rows, cols] = bf(dot(xt[...], dgu[:, cols], NN))
            up_cols = pl.ds(pl.multiple_of(ff + n * nn, nn), nn)
            dw_up[rows, cols] = bf(dot(xt[...], dgu[:, up_cols], NN))

        loop(ff // nn, cols_of)

    def tile_d(j):
        cols = pl.ds(pl.multiple_of(j * nb, nb), nb)
        mm = min(256, ff)

        def rows_of(m):
            rows = pl.ds(pl.multiple_of(m * mm, mm), mm)
            dw_down[rows, cols] = bf(dot(hid_t[rows, :], dyb[:, cols], NN))

        loop(ff // mm, rows_of)

    done = [0]

    def weights(n):
        lo, hi = done[0], min(done[0] + n, 2 * tiles)
        done[0] = hi
        a, b = min(lo, tiles), min(hi, tiles)
        if b > a:
            lax.fori_loop(a, b, lambda j, c: (tile_gu(j), c)[1], 0)
        a, b = max(lo, tiles) - tiles, max(hi, tiles) - tiles
        if b > a:
            lax.fori_loop(a, b, lambda j, c: (tile_d(j), c)[1], 0)

    for name, k in order():
        if name == "w":
            weights(k)
        else:
            {"h": stage_hidden, "a": stage_a, "b": stage_b, "c": stage_c, "own": stage_own, "o": stage_o, "c2": stage_c2,
             "o2": stage_o2, "r2": stage_r2, "g1": stage_g1, "r1": stage_r1, "end": stage_end}[name](k)
    weights(2 * tiles)
    for k in range(nk):
        sent(k)


ORDER = (
    "h0 a0 b0", "h1 a1 b1", "c0 own0", "h2 a2 b2", "c1 o0 own1", "h3 a3 b3", "c20 c2 own2 o1", "w1 o20 c21 own3", "w1 c3 r20 o2",
    "w1 o21 c22", "w1 g10 r21 o3", "w1 o22", "w1 g11 c23", "w1 r22", "w1 r10 o23", "w1 g12", "w1 r11 r23", "w2 r12 g13", "w3 r13",
    "w4 end0 end1", "end2 end3",
)


def order():
    return [(word[:-1], int(word[-1])) for words in ORDER for word in words.split()]


def write_out(*refs):
    n = (len(refs) - 1) // 2
    sem = refs[-1]
    copies = []
    for a, o in zip(refs[:n], refs[n : 2 * n]):
        parts = 4 if a.shape[0] * a.shape[1] > 2**21 else 1
        size = a.shape[0] // parts
        for i in range(parts):
            rows = pl.ds(i * size, size)
            copies.append(pltpu.make_async_copy(a.at[rows], o.at[rows], sem.at[len(copies)]))
    for c in copies:
        c.start()
    for c in copies:
        c.wait()


def solution(mesh):
    assert mesh.shape["tp"] == SIDE * SIDE

    def step(x, dy, gate, up, w_gate, w_up, w_down):
        rows, d = x.shape
        ff = gate.shape[1]
        nb = d // (2 * SIDE)
        chunks = chunk_rows(rows)
        nk = len(chunks)
        most = max(chunks)
        bf16, f32 = jnp.bfloat16, jnp.float32
        any_space = pl.BlockSpec(memory_space=pl.ANY)
        vmem = pl.BlockSpec(memory_space=pltpu.VMEM)
        shapes = [(rows, d), (d, ff), (d, ff), (ff, d)]
        flops = 2 * 6 * rows * d * ff
        results = pl.pallas_call(
            functools.partial(body, chunks),
            out_shape=[pltpu.VMEM(s, bf16) for s in shapes],
            in_specs=[any_space] * 7,
            out_specs=[vmem] * 4,
            scratch_shapes=[
                pltpu.VMEM((ff, d), bf16),
                pltpu.VMEM((d, 2 * ff), bf16),
                pltpu.VMEM((rows, 2 * ff), bf16),
                pltpu.VMEM((ff, rows), bf16),
                pltpu.VMEM((rows, d), bf16),
                pltpu.VMEM((2, most, ff), bf16),
                pltpu.VMEM((2, most, ff), bf16),
                pltpu.VMEM((2, rows, nb), bf16),
                pltpu.VMEM((nb, rows), bf16),
                *[pltpu.VMEM((4, rows // 2, nb), bf16) for _ in range(5)],
                pltpu.VMEM((4, rows // 2, nb), f32),
                pltpu.VMEM((2, 2, rows // 2, nb), f32),
                *[pltpu.VMEM((4, rows // (2 * SIDE), nb), bf16) for _ in range(5)],
                pltpu.SemaphoreType.DMA((5 + 3 * nk,)),
                pltpu.SemaphoreType.DMA((12, nk, 4)),
                pltpu.SemaphoreType.DMA((12, nk, 4)),
            ],
            compiler_params=pltpu.CompilerParams(
                collective_id=0, has_side_effects=True, vmem_limit_bytes=48 * 2**20
            ),
            cost_estimate=pl.CostEstimate(flops=flops, bytes_accessed=30 * 2**20, transcendentals=rows * ff),
            name="backward",
        )(x, dy, gate, up, w_gate, w_up, w_down)
        return pl.pallas_call(
            write_out,
            out_shape=[jax.ShapeDtypeStruct(s, bf16) for s in shapes],
            in_specs=[any_space] * 4,
            out_specs=[pl.BlockSpec(memory_space=pltpu.HBM)] * 4,
            scratch_shapes=[pltpu.SemaphoreType.DMA((16,))],
            compiler_params=pltpu.CompilerParams(vmem_limit_bytes=2**20),
            name="write_out",
        )(*results)

    tokens, columns, rows = P("dp", None), P(None, "tp"), P("tp", None)
    return jax.shard_map(
        step,
        mesh=mesh,
        in_specs=(tokens, tokens, P("dp", "tp"), P("dp", "tp"), columns, columns, rows),
        out_specs=(tokens, P("dp", "tp"), P("dp", "tp"), P(("dp", "tp"), None)),
        check_vma=False,
    )
```

```python
import functools
import math

import jax
import jax.numpy as jnp
from jax import lax
from jax.experimental import pallas as pl
from jax.experimental.pallas import tpu as pltpu
from jax.sharding import PartitionSpec as P

SIDE = 4
CHUNKS = (256, 512, 768, 512)
A, B, C, A2, B2, C2, G20, G21, R2, G10, G11, R1 = range(12)
NT = (((1,), (1,)), ((), ()))
NN = (((1,), (0,)), ((), ()))


def dot(a, b, dims):
    return lax.dot_general(a, b, dims, preferred_element_type=jnp.float32)


def chunk_rows(rows):
    return [rows * c // sum(CHUNKS) for c in CHUNKS]


def body(chunks, x, dy, gate, up, w_gate, w_up, w_down, dx, dw_gate, dw_up, dw_down,
         wd, wgu, dgu, hid_t, dyb, gub, xb, xt, st_a, st_b, r_a, r_bc, c_term, own,
         s2_a, s2_b, r2_a, r2_bc, lsem, ssem, rsem, end_sem):
    d = x.shape[1]
    ff = gate.shape[1]
    nb = d // (2 * SIDE)
    starts = [sum(chunks[:k]) for k in range(len(chunks))]
    t = lax.axis_index("tp")
    px, py = lax.div(t, SIDE), lax.rem(t, SIDE)

    def to(axis, s):
        step = 1 + (SIDE - 2) * s
        return lax.rem(px + (1 - axis) * step, SIDE) * SIDE + lax.rem(py + axis * step, SIDE)

    def on(axis):
        return px * (1 - axis) + py * axis

    def local(src, dst, i):
        return pltpu.make_async_copy(src, dst, lsem.at[i])

    def send(kind, recv, i, src, dst, axis):
        return pltpu.make_async_remote_copy(
            src_ref=src, dst_ref=dst, send_sem=ssem.at[kind], recv_sem=recv,
            device_id={"tp": to(axis, lax.rem(i, 2))}, device_id_type=pl.DeviceIdType.MESH,
        )

    def all_of(recv, ref):
        send(A, recv, 0, ref, ref, 0).wait_recv()

    def loop(n, f):
        lax.fori_loop(0, n, lambda i, c: (f(i), c)[1], 0)

    nk = len(chunks)
    wd_parts = 2
    slots = (0, max(chunks[::2]))

    def load_wd(n):
        rows = pl.ds(n * (ff // wd_parts), ff // wd_parts)
        return local(w_down.at[rows], wd.at[rows], n)

    def load_dy(k):
        rows = pl.ds(starts[k], chunks[k])
        return local(dy.at[rows], dyb.at[rows], 2 + k)

    def load_gu(k):
        rows, slot, sem = pl.ds(starts[k], chunks[k]), pl.ds(slots[k % 2], chunks[k]), 2 + nk + k
        return local(gate.at[rows], gub.at[0, slot], sem), local(up.at[rows], gub.at[1, slot], sem)

    def wait_gu(k):
        ref = gub.at[:, pl.ds(slots[k % 2], chunks[k])]
        local(ref, ref, 2 + nk + k).wait()

    def load_x(j, slot):
        return local(x.at[:, pl.ds(pl.multiple_of(j * nb, nb), nb)], xb.at[slot], 2 + 2 * nk + slot)

    def mod(v):
        return lax.rem(v, SIDE)

    def w_rows(h, n):
        return pl.ds(pl.multiple_of((h * SIDE + mod(on(h) + n)) * nb, nb), nb)

    def load_w(h, n):
        rows, sem = w_rows(h, n), 4 + 2 * nk + h * SIDE + n
        return local(w_gate.at[rows], wgu.at[rows, pl.ds(0, ff)], sem), local(w_up.at[rows], wgu.at[rows, pl.ds(ff, ff)], sem)

    def wait_w(h, n):
        ref = wgu.at[w_rows(h, n)]
        local(ref, ref, 4 + 2 * nk + h * SIDE + n).wait()

    def start(*copies):
        for c in copies:
            c.start()

    start(load_wd(0), load_dy(0), *load_gu(0), load_wd(1))

    def start_weights():
        start(*load_w(0, 2), *load_w(1, 2), *load_w(0, 1), *load_w(0, 3), *load_w(1, 1), *load_w(1, 3))

    def start_rest():
        if nk > 1:
            start(load_dy(1), *load_gu(1))
        start(*load_w(0, 0), *load_w(1, 0))
        start(*[load_dy(k) for k in range(2, nk)])
        start(load_x(0, 0), load_x(1, 1))

    barrier = pltpu.get_barrier_semaphore()
    for axis in range(2):
        for s in range(2):
            pl.semaphore_signal(barrier, inc=1, device_id={"tp": to(axis, s)}, device_id_type=pl.DeviceIdType.MESH)

    def ru(k):
        return chunks[k] // 2

    def rs(k):
        return chunks[k] // (2 * SIDE)

    def unit_rows(k, u):
        return pl.ds(starts[k] + u * ru(k), ru(k))

    def u1(k):
        return pl.ds(starts[k] // 2, ru(k))

    def u2(k):
        return pl.ds(starts[k] // (2 * SIDE), rs(k))

    def term(k, u, h, j):
        w = pl.ds(pl.multiple_of((h * SIDE + j) * nb, nb), nb)
        return dot(dgu[unit_rows(k, u), :], wgu[w, :], NT)

    def block(k, h, j):
        w = pl.ds(pl.multiple_of((h * SIDE + j) * nb, nb), nb)
        return dot(dgu[pl.ds(starts[k], chunks[k]), :], wgu[w, :], NT)

    def sub(k, q):
        return pl.ds(pl.multiple_of(starts[k] // 2 + q * rs(k), 16), rs(k))

    def region(k, u, h, j, q=None):
        cols = pl.ds(pl.multiple_of((h * SIDE + j) * nb, nb), nb)
        if q is None:
            return dx.at[pl.ds(pl.multiple_of(starts[k] + u * ru(k), 16), ru(k)), cols]
        return dx.at[pl.ds(pl.multiple_of(starts[k] + u * ru(k) + q * rs(k), 16), rs(k)), cols]

    def m_a(k, i, h):
        return send(A, rsem.at[k, h], i, st_a.at[i, u1(k)], r_a.at[i, u1(k)], h)

    def m_b(k, i, h):
        return send(B, rsem.at[k, 2 + h], i, st_b.at[i, u1(k)], r_bc.at[h, lax.rem(i, 2), u1(k)], h)

    def m_c(k, i, h):
        return send(C, rsem.at[k, 2 + h], i, r_a.at[i, u1(k)], r_bc.at[h, 2 + lax.rem(i, 2), u1(k)], h)

    def m_a2(k, i, h):
        return send(A2, rsem.at[k, 4 + h], i, s2_a.at[i, u2(k)], r2_a.at[i, u2(k)], 1 - h)

    def m_b2(k, i, h):
        return send(B2, rsem.at[k, 6 + h], i, s2_b.at[i, u2(k)], r2_bc.at[h, lax.rem(i, 2), u2(k)], 1 - h)

    def m_c2(k, i, h):
        return send(C2, rsem.at[k, 6 + h], i, r2_a.at[i, u2(k)], r2_bc.at[h, 2 + lax.rem(i, 2), u2(k)], 1 - h)

    def m_g2(k, i, h, s, n):
        where = region(k, s if n == 0 else 1 - s, h, on(h), on(1 - h))
        return send(G20 + n, rsem.at[k, (4 if n else 2) + h], i, where, where, 1 - h)

    def m_r2(k, i, h, s):
        where = region(k, s, h, on(h), mod(on(1 - h) + SIDE - 1 + 2 * s))
        return send(R2, rsem.at[k, 4 + h], i, where, where, 1 - h)

    def m_g1(k, i, h, s, n):
        where = region(k, s if n == 0 else 1 - s, h, on(h))
        return send(G10 + n, rsem.at[k, h] if n == 0 else end_sem, i, where, where, h)

    def m_r1(k, i, h, s):
        where = region(k, s, h, mod(on(h) + SIDE - 1 + 2 * s))
        return send(R1, end_sem, i, where, where, h)

    def hs(i):
        return lax.div(i, 2), lax.rem(i, 2)

    def bf(v):
        return v.astype(jnp.bfloat16)

    def f32(v):
        return v.astype(jnp.float32)

    def stage_hidden(k):
        nn = ff // wd_parts
        full = max((chunks[k] - 128) // 256, 0)
        last = chunks[k] - 256 * full
        load_dy(k).wait()
        wait_gu(k)
        if k == 0:
            start_weights()
        if k == 0 and full:
            for n in range(wd_parts):
                load_wd(n).wait()

        def tile(m, size):
            rows = pl.ds(pl.multiple_of(starts[k] + m * 256, 128), size)
            part = pl.ds(pl.multiple_of(slots[k % 2] + m * 256, 128), size)
            for n in range(wd_parts):
                cols = pl.ds(n * nn, nn)
                if k == 0 and not full:
                    load_wd(n).wait()
                dh = dot(dyb[rows, :], wd[cols, :], NT)
                g, v = f32(gub[0, part, cols]), f32(gub[1, part, cols])
                sg = 1.0 / (1.0 + jnp.exp(-g))
                silu = g * sg
                dgu[rows, cols] = bf(dh * v * (sg + silu * (1.0 - sg)))
                dgu[rows, pl.ds(ff + n * nn, nn)] = bf(dh * silu)
                hid_t[cols, rows] = bf(silu * v).T

        if full:
            loop(full, lambda m: tile(m, 256))
        tile(full, last)
        if k == 0:
            start_rest()
        if k + 2 < nk:
            for c in load_gu(k + 2):
                c.start()

    def stage_a(k):
        def half(h):
            if k == 0:
                wait_w(h, 2)
            both = bf(block(k, h, mod(on(h) + 2)))
            for s in range(2):
                st_a[2 * h + s, u1(k), :] = both[s * ru(k) : (s + 1) * ru(k)]
            if k == 0:
                pl.when(h == 0)(lambda: pl.semaphore_wait(barrier, 4))
            for s in range(2):
                m_a(k, 2 * h + s, h).start()

        loop(2, half)

    def stage_b(k):
        def each(i):
            h, s = hs(i)
            if k == 0:
                wait_w(h, 1 + 2 * s)
            j = mod(on(h) + 1 + 2 * s)
            st_b[i, u1(k), :] = bf(term(k, 1 - s, h, j))
            m_b(k, i, h).start()

        loop(4, each)

    def stage_ct(k):
        def each(i):
            h, s = hs(i)
            c_term[i, u1(k), :] = term(k, s, h, mod(on(h) + 1 + 2 * s))

        loop(4, each)

    def stage_c(k):
        def each(h):
            all_of(rsem.at[k, h], r_a.at[pl.ds(2 * h, 2), u1(k)])
            for s in range(2):
                i = 2 * h + s
                r_a[i, u1(k), :] = bf(c_term[i, u1(k), :] + f32(r_a[i, u1(k), :]))
                m_c(k, i, h).start()

        loop(2, each)

    def stage_own(k):
        def each(h):
            if k == 0:
                wait_w(h, 0)
            both = block(k, h, on(h))
            for u in range(2):
                own[h, u, u1(k), :] = both[u * ru(k) : (u + 1) * ru(k)]

        loop(2, each)

    def stage_o(k):
        def each(h):
            all_of(rsem.at[k, 2 + h], r_bc.at[h, :, u1(k)])
            for u in range(2):
                own[h, u, u1(k), :] += f32(r_bc[h, 2 + u, u1(k), :]) + f32(r_bc[h, 1 - u, u1(k), :])
            q = on(1 - h)
            for s in range(2):
                s2_a[2 * h + s, u2(k), :] = bf(own[h, s, sub(k, mod(q + 2)), :])
                m_a2(k, 2 * h + s, h).start()
            for s in range(2):
                s2_b[2 * h + s, u2(k), :] = bf(own[h, 1 - s, sub(k, mod(q + 1 + 2 * s)), :])
                m_b2(k, 2 * h + s, h).start()

        loop(2, each)

    def stage_c2(k):
        def each(h):
            all_of(rsem.at[k, 4 + h], r2_a.at[pl.ds(2 * h, 2), u2(k)])
            for s in range(2):
                i = 2 * h + s
                r2_a[i, u2(k), :] = bf(own[h, s, sub(k, mod(on(1 - h) + 1 + 2 * s)), :] + f32(r2_a[i, u2(k), :]))
                m_c2(k, i, h).start()

        loop(2, each)

    def stage_o2(k):
        def each(h):
            all_of(rsem.at[k, 6 + h], r2_bc.at[h, :, u2(k)])
            q = on(1 - h)
            for u in range(2):
                total = own[h, u, sub(k, q), :] + f32(r2_bc[h, 2 + u, u2(k), :]) + f32(r2_bc[h, 1 - u, u2(k), :])
                region(k, u, h, on(h), q)[...] = bf(total)
            for n in range(2):
                for s in range(2):
                    m_g2(k, 2 * h + s, h, s, n).start()

        loop(2, each)

    def stage_r2(k):
        def each(h):
            all_of(rsem.at[k, 2 + h], r2_a.at[pl.ds(2 * h, 2), u2(k)])
            for s in range(2):
                m_r2(k, 2 * h + s, h, s).start()

        loop(2, each)

    def stage_g1(k):
        def each(h):
            all_of(rsem.at[k, 4 + h], r2_bc.at[h, :, u2(k)])
            for n in range(2):
                for s in range(2):
                    m_g1(k, 2 * h + s, h, s, n).start()

        loop(2, each)

    def stage_r1(k):
        def each(h):
            all_of(rsem.at[k, h], r_a.at[pl.ds(2 * h, 2), u1(k)])
            for s in range(2):
                m_r1(k, 2 * h + s, h, s).start()

        loop(2, each)

    def finish():
        all_of(end_sem, r_bc)
        for kinds, ref in (((A, B, C, G10, G11, R1), st_a), ((A2, B2, C2, G20, G21, R2), s2_a)):
            for kind in kinds:
                send(kind, end_sem, 0, ref, ref, 0).wait_send()

    tiles = d // nb

    def tile_gu(j):
        slot = lax.rem(j, 2)
        load_x(j, slot).wait()
        xt[...] = xb[slot].T
        pl.when(j + 2 < tiles)(lambda: load_x(j + 2, slot).start())
        nn = min(256, ff)
        rows = pl.ds(pl.multiple_of(j * nb, nb), nb)

        def cols_of(n):
            cols = pl.ds(pl.multiple_of(n * nn, nn), nn)
            dw_gate[rows, cols] = bf(dot(xt[...], dgu[:, cols], NN))
            up_cols = pl.ds(pl.multiple_of(ff + n * nn, nn), nn)
            dw_up[rows, cols] = bf(dot(xt[...], dgu[:, up_cols], NN))

        loop(ff // nn, cols_of)

    def tile_d(j):
        cols = pl.ds(pl.multiple_of(j * nb, nb), nb)
        mm = min(256, ff)

        def rows_of(m):
            rows = pl.ds(pl.multiple_of(m * mm, mm), mm)
            dw_down[rows, cols] = bf(dot(hid_t[rows, :], dyb[:, cols], NN))

        loop(ff // mm, rows_of)

    done = [0]

    def weights(n):
        lo, hi = done[0], min(done[0] + n, 2 * tiles)
        done[0] = hi
        a, b = min(lo, tiles), min(hi, tiles)
        if b > a:
            lax.fori_loop(a, b, lambda j, c: (tile_gu(j), c)[1], 0)
        a, b = max(lo, tiles) - tiles, max(hi, tiles) - tiles
        if b > a:
            lax.fori_loop(a, b, lambda j, c: (tile_d(j), c)[1], 0)

    for name, k in order():
        if name == "w":
            weights(k)
        else:
            {"h": stage_hidden, "a": stage_a, "b": stage_b, "ct": stage_ct, "c": stage_c, "own": stage_own, "o": stage_o, "c2": stage_c2,
             "o2": stage_o2, "r2": stage_r2, "g1": stage_g1, "r1": stage_r1}[name](k)
    weights(2 * tiles)
    finish()


ORDER = (
    "h0 a0 b0 h1", "a1 b1 h2 a2", "own0 ct2 ct1 h3", "c1 ct0 ct3 c0", "own1 c2 w1 b2", "w1 o1 own2 a3", "o0 own3 c21 o2",
    "b3 w1 c20 c22", "o21 c3 o20 o22", "r21 r20 o3 r22", "g11 w1 c23 g10", "w1 g12 w1 w1", "o23 r11 w1 w1", "r10 r23 w1 w1",
    "w1 r12 g13 r13", "w1 w1 w1 w1",
)


def order():
    return [(word[:-1], int(word[-1])) for words in ORDER for word in words.split()]


def write_out(*refs):
    n = (len(refs) - 1) // 2
    sem = refs[-1]
    copies = []
    for a, o in zip(refs[:n], refs[n : 2 * n]):
        parts = 4 if a.shape[0] * a.shape[1] > 2**21 else 1
        size = a.shape[0] // parts
        for i in range(parts):
            rows = pl.ds(i * size, size)
            copies.append(pltpu.make_async_copy(a.at[rows], o.at[rows], sem.at[len(copies)]))
    for c in copies:
        c.start()
    for c in copies:
        c.wait()


def solution(mesh):
    assert mesh.shape["tp"] == SIDE * SIDE

    def step(x, dy, gate, up, w_gate, w_up, w_down):
        rows, d = x.shape
        ff = gate.shape[1]
        nb = d // (2 * SIDE)
        chunks = chunk_rows(rows)
        nk = len(chunks)
        bf16, f32 = jnp.bfloat16, jnp.float32
        any_space = pl.BlockSpec(memory_space=pl.ANY)
        vmem = pl.BlockSpec(memory_space=pltpu.VMEM)
        shapes = [(rows, d), (d, ff), (d, ff), (ff, d)]
        flops = 2 * 6 * rows * d * ff
        results = pl.pallas_call(
            functools.partial(body, chunks),
            out_shape=[pltpu.VMEM(s, bf16) for s in shapes],
            in_specs=[any_space] * 7,
            out_specs=[vmem] * 4,
            scratch_shapes=[
                pltpu.VMEM((ff, d), bf16),
                pltpu.VMEM((d, 2 * ff), bf16),
                pltpu.VMEM((rows, 2 * ff), bf16),
                pltpu.VMEM((ff, rows), bf16),
                pltpu.VMEM((rows, d), bf16),
                pltpu.VMEM((2, max(chunks[::2]) + max(chunks[1::2]), ff), bf16),
                pltpu.VMEM((2, rows, nb), bf16),
                pltpu.VMEM((nb, rows), bf16),
                *[pltpu.VMEM((4, rows // 2, nb), bf16) for _ in range(3)],
                pltpu.VMEM((2, 4, rows // 2, nb), bf16),
                pltpu.VMEM((4, rows // 2, nb), f32),
                pltpu.VMEM((2, 2, rows // 2, nb), f32),
                *[pltpu.VMEM((4, rows // (2 * SIDE), nb), bf16) for _ in range(3)],
                pltpu.VMEM((2, 4, rows // (2 * SIDE), nb), bf16),
                pltpu.SemaphoreType.DMA((4 + 2 * nk + 2 * SIDE,)),
                pltpu.SemaphoreType.DMA((12,)),
                pltpu.SemaphoreType.DMA((nk, 8)),
                pltpu.SemaphoreType.DMA,
            ],
            compiler_params=pltpu.CompilerParams(
                collective_id=0, has_side_effects=True, vmem_limit_bytes=50944 * 2**10
            ),
            cost_estimate=pl.CostEstimate(flops=flops, bytes_accessed=30 * 2**20, transcendentals=rows * ff),
            name="backward",
        )(x, dy, gate, up, w_gate, w_up, w_down)
        return pl.pallas_call(
            write_out,
            out_shape=[jax.ShapeDtypeStruct(s, bf16) for s in shapes],
            in_specs=[any_space] * 4,
            out_specs=[pl.BlockSpec(memory_space=pltpu.HBM)] * 4,
            scratch_shapes=[pltpu.SemaphoreType.DMA((16,))],
            compiler_params=pltpu.CompilerParams(vmem_limit_bytes=2**20),
            name="write_out",
        )(*results)

    tokens, columns, rows = P("dp", None), P(None, "tp"), P("tp", None)
    return jax.shard_map(
        step,
        mesh=mesh,
        in_specs=(tokens, tokens, P("dp", "tp"), P("dp", "tp"), columns, columns, rows),
        out_specs=(tokens, P("dp", "tp"), P("dp", "tp"), P(("dp", "tp"), None)),
        check_vma=False,
    )
```

```python
import functools
import math

import jax
import jax.numpy as jnp
from jax import lax
from jax.experimental import pallas as pl
from jax.experimental.pallas import tpu as pltpu
from jax.sharding import PartitionSpec as P

SIDE = 4
CHUNKS = (256, 384, 640, 768)
A, B, C, AB2, C2, G20, G21, R2, G10, G11, R1 = range(11)
NT = (((1,), (1,)), ((), ()))
NN = (((1,), (0,)), ((), ()))


def dot(a, b, dims):
    return lax.dot_general(a, b, dims, preferred_element_type=jnp.float32)


def chunk_rows(rows):
    return [rows * c // sum(CHUNKS) for c in CHUNKS]


def body(chunks, x, dy, gate, up, w_gate, w_up, w_down, dx, dw_gate, dw_up, dw_down,
         wd, wgu, dgu, hid_t, dyb, gub, xb, xt, st_a, st_b, r_a, r_bc, c_term, own,
         s2_ab, r2_ab, r2_c, lsem, ssem, rsem, end_sem):
    d = x.shape[1]
    ff = gate.shape[1]
    nb = d // (2 * SIDE)
    starts = [sum(chunks[:k]) for k in range(len(chunks))]
    t = lax.axis_index("tp")
    px, py = lax.div(t, SIDE), lax.rem(t, SIDE)

    def to(axis, s):
        step = 1 + (SIDE - 2) * s
        return lax.rem(px + (1 - axis) * step, SIDE) * SIDE + lax.rem(py + axis * step, SIDE)

    def on(axis):
        return px * (1 - axis) + py * axis

    def local(src, dst, i):
        return pltpu.make_async_copy(src, dst, lsem.at[i])

    def send(kind, recv, i, src, dst, axis):
        return pltpu.make_async_remote_copy(
            src_ref=src, dst_ref=dst, send_sem=ssem.at[kind], recv_sem=recv,
            device_id={"tp": to(axis, lax.rem(i, 2))}, device_id_type=pl.DeviceIdType.MESH,
        )

    def all_of(recv, ref):
        send(A, recv, 0, ref, ref, 0).wait_recv()

    def loop(n, f):
        lax.fori_loop(0, n, lambda i, c: (f(i), c)[1], 0)

    nk = len(chunks)
    wd_parts = 2
    slots = (0, max(chunks[::2]))

    def load_wd(n):
        rows = pl.ds(n * (ff // wd_parts), ff // wd_parts)
        return local(w_down.at[rows], wd.at[rows], n)

    def load_dy(k):
        rows = pl.ds(starts[k], chunks[k])
        return local(dy.at[rows], dyb.at[rows], 2 + k)

    def load_gu(k):
        rows, slot, sem = pl.ds(starts[k], chunks[k]), pl.ds(slots[k % 2], chunks[k]), 2 + nk + k
        return local(gate.at[rows], gub.at[0, slot], sem), local(up.at[rows], gub.at[1, slot], sem)

    def wait_gu(k):
        ref = gub.at[:, pl.ds(slots[k % 2], chunks[k])]
        local(ref, ref, 2 + nk + k).wait()

    def load_x(j, slot):
        return local(x.at[:, pl.ds(pl.multiple_of(j * nb, nb), nb)], xb.at[slot], 2 + 2 * nk + slot)

    def mod(v):
        return lax.rem(v, SIDE)

    def w_rows(h, n):
        return pl.ds(pl.multiple_of((h * SIDE + mod(on(h) + n)) * nb, nb), nb)

    def load_w(h, n):
        rows, sem = w_rows(h, n), 4 + 2 * nk + h * SIDE + n
        return local(w_gate.at[rows], wgu.at[rows, pl.ds(0, ff)], sem), local(w_up.at[rows], wgu.at[rows, pl.ds(ff, ff)], sem)

    def wait_w(h, n):
        ref = wgu.at[w_rows(h, n)]
        local(ref, ref, 4 + 2 * nk + h * SIDE + n).wait()

    def start(*copies):
        for c in copies:
            c.start()

    start(load_wd(0), load_dy(0), *load_gu(0), load_wd(1))

    def start_weights():
        start(*load_w(0, 2), *load_w(1, 2), *load_w(0, 1), *load_w(0, 3), *load_w(1, 1), *load_w(1, 3))

    def start_rest():
        if nk > 1:
            start(load_dy(1), *load_gu(1))
        start(*load_w(0, 0), *load_w(1, 0))
        start(*[load_dy(k) for k in range(2, nk)])
        start(load_x(0, 0), load_x(1, 1))

    barrier = pltpu.get_barrier_semaphore()
    for axis in range(2):
        for s in range(2):
            pl.semaphore_signal(barrier, inc=1, device_id={"tp": to(axis, s)}, device_id_type=pl.DeviceIdType.MESH)

    def ru(k):
        return chunks[k] // 2

    def rs(k):
        return chunks[k] // (2 * SIDE)

    def unit_rows(k, u):
        return pl.ds(starts[k] + u * ru(k), ru(k))

    def u1(k):
        return pl.ds(starts[k] // 2, ru(k))

    def u2(k):
        return pl.ds(starts[k] // (2 * SIDE), rs(k))

    def term(k, u, h, j):
        w = pl.ds(pl.multiple_of((h * SIDE + j) * nb, nb), nb)
        return dot(dgu[unit_rows(k, u), :], wgu[w, :], NT)

    def block(k, h, j):
        w = pl.ds(pl.multiple_of((h * SIDE + j) * nb, nb), nb)
        return dot(dgu[pl.ds(starts[k], chunks[k]), :], wgu[w, :], NT)

    def sub(k, q):
        return pl.ds(pl.multiple_of(starts[k] // 2 + q * rs(k), 16), rs(k))

    def region(k, u, h, j, q=None):
        cols = pl.ds(pl.multiple_of((h * SIDE + j) * nb, nb), nb)
        if q is None:
            return dx.at[pl.ds(pl.multiple_of(starts[k] + u * ru(k), 16), ru(k)), cols]
        return dx.at[pl.ds(pl.multiple_of(starts[k] + u * ru(k) + q * rs(k), 16), rs(k)), cols]

    def m_a(k, i, h):
        return send(A, rsem.at[k, h], i, st_a.at[i, u1(k)], r_a.at[i, u1(k)], h)

    def m_b(k, i, h):
        return send(B, rsem.at[k, 2 + h], i, st_b.at[i, u1(k)], r_bc.at[h, lax.rem(i, 2), u1(k)], h)

    def m_c(k, i, h):
        return send(C, rsem.at[k, 2 + h], i, r_a.at[i, u1(k)], r_bc.at[h, 2 + lax.rem(i, 2), u1(k)], h)

    def m_ab2(k, i, h):
        return send(AB2, rsem.at[k, 4 + h], i, s2_ab.at[i, :, u2(k)], r2_ab.at[i, :, u2(k)], 1 - h)

    def m_c2(k, i, h):
        return send(C2, rsem.at[k, 6 + h], i, r2_ab.at[i, 0, u2(k)], r2_c.at[i, u2(k)], 1 - h)

    def m_g2(k, i, h, s, n):
        where = region(k, s if n == 0 else 1 - s, h, on(h), on(1 - h))
        return send(G20 + n, rsem.at[k, (4 if n else 2) + h], i, where, where, 1 - h)

    def m_r2(k, i, h, s):
        where = region(k, s, h, on(h), mod(on(1 - h) + SIDE - 1 + 2 * s))
        return send(R2, rsem.at[k, 4 + h], i, where, where, 1 - h)

    def m_g1(k, i, h, s, n):
        where = region(k, s if n == 0 else 1 - s, h, on(h))
        return send(G10 + n, rsem.at[k, h] if n == 0 else end_sem, i, where, where, h)

    def m_r1(k, i, h, s):
        where = region(k, s, h, mod(on(h) + SIDE - 1 + 2 * s))
        return send(R1, end_sem, i, where, where, h)

    def bf(v):
        return v.astype(jnp.bfloat16)

    def f32(v):
        return v.astype(jnp.float32)

    def stage_hidden(k):
        nn = ff // wd_parts
        full = max((chunks[k] - 128) // 256, 0)
        last = chunks[k] - 256 * full
        load_dy(k).wait()
        wait_gu(k)
        if k == 0:
            start_weights()
        if k == 0 and full:
            for n in range(wd_parts):
                load_wd(n).wait()

        def tile(m, size):
            rows = pl.ds(pl.multiple_of(starts[k] + m * 256, 128), size)
            part = pl.ds(pl.multiple_of(slots[k % 2] + m * 256, 128), size)
            for n in range(wd_parts):
                cols = pl.ds(n * nn, nn)
                if k == 0 and not full:
                    load_wd(n).wait()
                dh = dot(dyb[rows, :], wd[cols, :], NT)
                g, v = f32(gub[0, part, cols]), f32(gub[1, part, cols])
                sg = 1.0 / (1.0 + jnp.exp(-g))
                silu = g * sg
                dgu[rows, cols] = bf(dh * v * (sg + silu * (1.0 - sg)))
                dgu[rows, pl.ds(ff + n * nn, nn)] = bf(dh * silu)
                hid_t[cols, rows] = bf(silu * v).T

        if full:
            loop(full, lambda m: tile(m, 256))
        tile(full, last)
        if k == 0:
            start_rest()
        if k + 2 < nk:
            for c in load_gu(k + 2):
                c.start()

    def stage_a(k):
        def half(h):
            if k == 0:
                wait_w(h, 2)
            both = bf(block(k, h, mod(on(h) + 2)))
            for s in range(2):
                st_a[2 * h + s, u1(k), :] = both[s * ru(k) : (s + 1) * ru(k)]
            if k == 0:
                pl.when(h == 0)(lambda: pl.semaphore_wait(barrier, 4))
            for s in range(2):
                m_a(k, 2 * h + s, h).start()

        loop(2, half)

    def stage_b(k):
        def each(h):
            for s in range(2):
                if k == 0:
                    wait_w(h, 1 + 2 * s)
                st_b[2 * h + s, u1(k), :] = bf(term(k, 1 - s, h, mod(on(h) + 1 + 2 * s)))
            for s in range(2):
                m_b(k, 2 * h + s, h).start()

        loop(2, each)

    def stage_ct(k):
        def each(h):
            for s in range(2):
                c_term[2 * h + s, u1(k), :] = term(k, s, h, mod(on(h) + 1 + 2 * s))

        loop(2, each)

    def stage_c(k):
        def each(h):
            all_of(rsem.at[k, h], r_a.at[pl.ds(2 * h, 2), u1(k)])
            for s in range(2):
                i = 2 * h + s
                r_a[i, u1(k), :] = bf(c_term[i, u1(k), :] + f32(r_a[i, u1(k), :]))
                m_c(k, i, h).start()

        loop(2, each)

    def stage_own(k):
        def each(h):
            if k == 0:
                wait_w(h, 0)
            both = block(k, h, on(h))
            for u in range(2):
                own[h, u, u1(k), :] = both[u * ru(k) : (u + 1) * ru(k)]

        loop(2, each)

    def stage_o(k):
        def each(h):
            all_of(rsem.at[k, 2 + h], r_bc.at[h, :, u1(k)])
            for u in range(2):
                own[h, u, u1(k), :] += f32(r_bc[h, 2 + u, u1(k), :]) + f32(r_bc[h, 1 - u, u1(k), :])
            q = on(1 - h)
            for s in range(2):
                s2_ab[2 * h + s, 0, u2(k), :] = bf(own[h, s, sub(k, mod(q + 2)), :])
                s2_ab[2 * h + s, 1, u2(k), :] = bf(own[h, 1 - s, sub(k, mod(q + 1 + 2 * s)), :])
            for s in range(2):
                m_ab2(k, 2 * h + s, h).start()

        loop(2, each)

    def stage_c2(k):
        def each(h):
            all_of(rsem.at[k, 4 + h], r2_ab.at[pl.ds(2 * h, 2), :, u2(k)])
            for s in range(2):
                i = 2 * h + s
                r2_ab[i, 0, u2(k), :] = bf(own[h, s, sub(k, mod(on(1 - h) + 1 + 2 * s)), :] + f32(r2_ab[i, 0, u2(k), :]))
                m_c2(k, i, h).start()

        loop(2, each)

    def stage_o2(k):
        def each(h):
            all_of(rsem.at[k, 6 + h], r2_c.at[pl.ds(2 * h, 2), u2(k)])
            q = on(1 - h)
            for u in range(2):
                total = own[h, u, sub(k, q), :] + f32(r2_c[2 * h + u, u2(k), :]) + f32(r2_ab[2 * h + 1 - u, 1, u2(k), :])
                region(k, u, h, on(h), q)[...] = bf(total)
            for n in range(2):
                for s in range(2):
                    m_g2(k, 2 * h + s, h, s, n).start()

        loop(2, each)

    def stage_r2(k):
        def each(h):
            all_of(rsem.at[k, 2 + h], r2_c.at[pl.ds(2 * h, 2), u2(k)])
            for s in range(2):
                m_r2(k, 2 * h + s, h, s).start()

        loop(2, each)

    def stage_g1(k):
        def each(h):
            all_of(rsem.at[k, 4 + h], r2_ab.at[pl.ds(2 * h, 2), :, u2(k)])
            for n in range(2):
                for s in range(2):
                    m_g1(k, 2 * h + s, h, s, n).start()

        loop(2, each)

    def stage_r1(k):
        def each(h):
            all_of(rsem.at[k, h], r_a.at[pl.ds(2 * h, 2), u1(k)])
            for s in range(2):
                m_r1(k, 2 * h + s, h, s).start()

        loop(2, each)

    def finish():
        all_of(end_sem, r_bc)
        for kinds, ref in (((A, B, C, G10, G11, R1), st_a), ((C2, G20, G21, R2), r2_c), ((AB2,), s2_ab)):
            for kind in kinds:
                send(kind, end_sem, 0, ref, ref, 0).wait_send()

    tiles = d // nb

    def tile_gu(j):
        slot = lax.rem(j, 2)
        load_x(j, slot).wait()
        xt[...] = xb[slot].T
        pl.when(j + 2 < tiles)(lambda: load_x(j + 2, slot).start())
        nn = min(256, ff)
        rows = pl.ds(pl.multiple_of(j * nb, nb), nb)

        def cols_of(n):
            cols = pl.ds(pl.multiple_of(n * nn, nn), nn)
            dw_gate[rows, cols] = bf(dot(xt[...], dgu[:, cols], NN))
            up_cols = pl.ds(pl.multiple_of(ff + n * nn, nn), nn)
            dw_up[rows, cols] = bf(dot(xt[...], dgu[:, up_cols], NN))

        loop(ff // nn, cols_of)

    def tile_d(j):
        cols = pl.ds(pl.multiple_of(j * nb, nb), nb)
        mm = min(256, ff)

        def rows_of(m):
            rows = pl.ds(pl.multiple_of(m * mm, mm), mm)
            dw_down[rows, cols] = bf(dot(hid_t[rows, :], dyb[:, cols], NN))

        loop(ff // mm, rows_of)

    done = [0]

    def weights(n):
        lo, hi = done[0], min(done[0] + n, 2 * tiles)
        done[0] = hi
        a, b = min(lo, tiles), min(hi, tiles)
        if b > a:
            lax.fori_loop(a, b, lambda j, c: (tile_gu(j), c)[1], 0)
        a, b = max(lo, tiles) - tiles, max(hi, tiles) - tiles
        if b > a:
            lax.fori_loop(a, b, lambda j, c: (tile_d(j), c)[1], 0)

    for name, k in order():
        if name == "w":
            weights(k)
        else:
            {"h": stage_hidden, "a": stage_a, "b": stage_b, "ct": stage_ct, "c": stage_c, "own": stage_own, "o": stage_o, "c2": stage_c2,
             "o2": stage_o2, "r2": stage_r2, "g1": stage_g1, "r1": stage_r1}[name](k)
    weights(2 * tiles)
    finish()


ORDER = (
    "h0 a0 b0 h1", "a1 b1 ct0 c0", "h2 a2 h3 own0", "o0 a3 b3 ct2", "ct1 c20 w1 w1", "c1 ct3 own1 own2", "c2 o20 w1 o1",
    "b2 r20 own3 c21", "c3 o2 o21 g10", "w1 w1 w1 c22", "o3 w1 r21 r10", "w1 o22 w1 c23", "g11 w1 r22 w1", "o23 r11 r23 g12",
    "w1 w1 g13 w1", "w1 w1 r12 r13",
)


def order():
    return [(word[:-1], int(word[-1])) for words in ORDER for word in words.split()]


def write_out(*refs):
    n = (len(refs) - 1) // 2
    sem = refs[-1]
    copies = []
    for a, o in zip(refs[:n], refs[n : 2 * n]):
        parts = 4 if a.shape[0] * a.shape[1] > 2**21 else 1
        size = a.shape[0] // parts
        for i in range(parts):
            rows = pl.ds(i * size, size)
            copies.append(pltpu.make_async_copy(a.at[rows], o.at[rows], sem.at[len(copies)]))
    for c in copies:
        c.start()
    for c in copies:
        c.wait()


def solution(mesh):
    assert mesh.shape["tp"] == SIDE * SIDE

    def step(x, dy, gate, up, w_gate, w_up, w_down):
        rows, d = x.shape
        ff = gate.shape[1]
        nb = d // (2 * SIDE)
        chunks = chunk_rows(rows)
        nk = len(chunks)
        bf16, f32 = jnp.bfloat16, jnp.float32
        any_space = pl.BlockSpec(memory_space=pl.ANY)
        vmem = pl.BlockSpec(memory_space=pltpu.VMEM)
        shapes = [(rows, d), (d, ff), (d, ff), (ff, d)]
        flops = 2 * 6 * rows * d * ff
        results = pl.pallas_call(
            functools.partial(body, chunks),
            out_shape=[pltpu.VMEM(s, bf16) for s in shapes],
            in_specs=[any_space] * 7,
            out_specs=[vmem] * 4,
            scratch_shapes=[
                pltpu.VMEM((ff, d), bf16),
                pltpu.VMEM((d, 2 * ff), bf16),
                pltpu.VMEM((rows, 2 * ff), bf16),
                pltpu.VMEM((ff, rows), bf16),
                pltpu.VMEM((rows, d), bf16),
                pltpu.VMEM((2, max(chunks[::2]) + max(chunks[1::2]), ff), bf16),
                pltpu.VMEM((2, rows, nb), bf16),
                pltpu.VMEM((nb, rows), bf16),
                *[pltpu.VMEM((4, rows // 2, nb), bf16) for _ in range(3)],
                pltpu.VMEM((2, 4, rows // 2, nb), bf16),
                pltpu.VMEM((4, rows // 2, nb), f32),
                pltpu.VMEM((2, 2, rows // 2, nb), f32),
                *[pltpu.VMEM((4, 2, rows // (2 * SIDE), nb), bf16) for _ in range(2)],
                pltpu.VMEM((4, rows // (2 * SIDE), nb), bf16),
                pltpu.SemaphoreType.DMA((4 + 2 * nk + 2 * SIDE,)),
                pltpu.SemaphoreType.DMA((11,)),
                pltpu.SemaphoreType.DMA((nk, 8)),
                pltpu.SemaphoreType.DMA,
            ],
            compiler_params=pltpu.CompilerParams(
                collective_id=0, has_side_effects=True, vmem_limit_bytes=50944 * 2**10
            ),
            cost_estimate=pl.CostEstimate(flops=flops, bytes_accessed=30 * 2**20, transcendentals=rows * ff),
            name="backward",
        )(x, dy, gate, up, w_gate, w_up, w_down)
        return pl.pallas_call(
            write_out,
            out_shape=[jax.ShapeDtypeStruct(s, bf16) for s in shapes],
            in_specs=[any_space] * 4,
            out_specs=[pl.BlockSpec(memory_space=pltpu.HBM)] * 4,
            scratch_shapes=[pltpu.SemaphoreType.DMA((16,))],
            compiler_params=pltpu.CompilerParams(vmem_limit_bytes=2**20),
            name="write_out",
        )(*results)

    tokens, columns, rows = P("dp", None), P(None, "tp"), P("tp", None)
    return jax.shard_map(
        step,
        mesh=mesh,
        in_specs=(tokens, tokens, P("dp", "tp"), P("dp", "tp"), columns, columns, rows),
        out_specs=(tokens, P("dp", "tp"), P("dp", "tp"), P(("dp", "tp"), None)),
        check_vma=False,
    )
```

```python
import functools
import math

import jax
import jax.numpy as jnp
from jax import lax
from jax.experimental import pallas as pl
from jax.experimental.pallas import tpu as pltpu
from jax.sharding import PartitionSpec as P

SIDE = 4
CHUNKS = (256, 384, 640, 768)
A, B, C, AB2, C2, G20, G21, R2, G10, G11, R1 = range(11)
NT = (((1,), (1,)), ((), ()))
NN = (((1,), (0,)), ((), ()))


def dot(a, b, dims):
    return lax.dot_general(a, b, dims, preferred_element_type=jnp.float32)


def chunk_rows(rows):
    return [rows * c // sum(CHUNKS) for c in CHUNKS]


def body(chunks, x, dy, gate, up, w_gate, w_up, w_down, dx, dw_gate, dw_up, dw_down,
         wd, wgu, dgu, hid_t, dyb, gub, xb, xt, st_a, st_b, r_a, r_bc, c_term, own,
         s2_ab, r2_ab, r2_c, lsem, ssem, rsem, end_sem):
    d = x.shape[1]
    ff = gate.shape[1]
    nb = d // (2 * SIDE)
    starts = [sum(chunks[:k]) for k in range(len(chunks))]
    t = lax.axis_index("tp")
    px, py = lax.div(t, SIDE), lax.rem(t, SIDE)

    def to(axis, s):
        step = 1 + (SIDE - 2) * s
        return lax.rem(px + (1 - axis) * step, SIDE) * SIDE + lax.rem(py + axis * step, SIDE)

    def on(axis):
        return px * (1 - axis) + py * axis

    def local(src, dst, i):
        return pltpu.make_async_copy(src, dst, lsem.at[i])

    def send(kind, recv, i, src, dst, axis):
        return pltpu.make_async_remote_copy(
            src_ref=src, dst_ref=dst, send_sem=ssem.at[kind], recv_sem=recv,
            device_id={"tp": to(axis, lax.rem(i, 2))}, device_id_type=pl.DeviceIdType.MESH,
        )

    def all_of(recv, ref):
        send(A, recv, 0, ref, ref, 0).wait_recv()

    def loop(n, f):
        lax.fori_loop(0, n, lambda i, c: (f(i), c)[1], 0)

    nk = len(chunks)
    wd_parts = 2
    slots = (0, max(chunks[::2]))

    def load_wd(n):
        rows = pl.ds(n * (ff // wd_parts), ff // wd_parts)
        return local(w_down.at[rows], wd.at[rows], n)

    def load_dy(k):
        rows = pl.ds(starts[k], chunks[k])
        return local(dy.at[rows], dyb.at[rows], 2 + (k if k < 2 else 0 if k == 2 else k - 1))

    def load_gu(k):
        rows, slot, sem = pl.ds(starts[k], chunks[k]), pl.ds(slots[k % 2], chunks[k]), 1 + nk + k % 2
        return local(gate.at[rows], gub.at[0, slot], sem), local(up.at[rows], gub.at[1, slot], sem)

    def wait_gu(k):
        ref = gub.at[:, pl.ds(slots[k % 2], chunks[k])]
        local(ref, ref, 1 + nk + k % 2).wait()

    def load_x(j, slot):
        return local(x.at[:, pl.ds(pl.multiple_of(j * nb, nb), nb)], xb.at[slot], slot)

    def mod(v):
        return lax.rem(v, SIDE)

    def w_rows(h, n):
        return pl.ds(pl.multiple_of((h * SIDE + mod(on(h) + n)) * nb, nb), nb)

    def load_w(h, n):
        rows, sem = w_rows(h, n), 3 + nk + h * SIDE + n
        return local(w_gate.at[rows], wgu.at[rows, pl.ds(0, ff)], sem), local(w_up.at[rows], wgu.at[rows, pl.ds(ff, ff)], sem)

    def wait_w(h, n):
        ref = wgu.at[w_rows(h, n)]
        local(ref, ref, 3 + nk + h * SIDE + n).wait()

    def start(*copies):
        for c in copies:
            c.start()

    start(load_wd(0), load_dy(0), *load_gu(0), load_wd(1))

    def start_weights():
        start(*load_w(0, 2), *load_w(1, 2), *load_w(0, 1), *load_w(0, 3), *load_w(1, 1), *load_w(1, 3))

    def start_rest():
        if nk > 1:
            start(load_dy(1), *load_gu(1))
        start(*load_w(0, 0), *load_w(1, 0))
        start(*[load_dy(k) for k in range(2, nk)])
        start(load_x(0, 0), load_x(1, 1))

    barrier = pltpu.get_barrier_semaphore()
    for axis in range(2):
        for s in range(2):
            pl.semaphore_signal(barrier, inc=1, device_id={"tp": to(axis, s)}, device_id_type=pl.DeviceIdType.MESH)

    def ru(k):
        return chunks[k] // 2

    def rs(k):
        return chunks[k] // (2 * SIDE)

    def unit_rows(k, u):
        return pl.ds(starts[k] + u * ru(k), ru(k))

    def u1(k):
        return pl.ds(starts[k] // 2, ru(k))

    def u2(k):
        return pl.ds(starts[k] // (2 * SIDE), rs(k))

    def term(k, u, h, j):
        w = pl.ds(pl.multiple_of((h * SIDE + j) * nb, nb), nb)
        return dot(dgu[unit_rows(k, u), :], wgu[w, :], NT)

    def block(k, h, j):
        w = pl.ds(pl.multiple_of((h * SIDE + j) * nb, nb), nb)
        return dot(dgu[pl.ds(starts[k], chunks[k]), :], wgu[w, :], NT)

    def sub(k, q):
        return pl.ds(pl.multiple_of(starts[k] // 2 + q * rs(k), 16), rs(k))

    def region(k, u, h, j, q=None):
        cols = pl.ds(pl.multiple_of((h * SIDE + j) * nb, nb), nb)
        if q is None:
            return dx.at[pl.ds(pl.multiple_of(starts[k] + u * ru(k), 16), ru(k)), cols]
        return dx.at[pl.ds(pl.multiple_of(starts[k] + u * ru(k) + q * rs(k), 16), rs(k)), cols]

    def m_a(k, i, h):
        return send(A, rsem.at[k, h], i, st_a.at[i, u1(k)], r_a.at[i, u1(k)], h)

    def m_b(k, i, h):
        return send(B, rsem.at[k, 2 + h], i, st_b.at[i, u1(k)], r_bc.at[h, lax.rem(i, 2), u1(k)], h)

    def m_c(k, i, h):
        return send(C, rsem.at[k, 2 + h], i, r_a.at[i, u1(k)], r_bc.at[h, 2 + lax.rem(i, 2), u1(k)], h)

    def m_ab2(k, i, h):
        return send(AB2, rsem.at[k, 4 + h], i, s2_ab.at[i, :, u2(k)], r2_ab.at[i, :, u2(k)], 1 - h)

    def m_c2(k, i, h):
        return send(C2, rsem.at[k, 6 + h], i, r2_ab.at[i, 0, u2(k)], r2_c.at[i, u2(k)], 1 - h)

    def m_g2(k, i, h, s, n):
        where = region(k, s if n == 0 else 1 - s, h, on(h), on(1 - h))
        return send(G20 + n, rsem.at[k, (4 if n else 2) + h], i, where, where, 1 - h)

    def m_r2(k, i, h, s):
        where = region(k, s, h, on(h), mod(on(1 - h) + SIDE - 1 + 2 * s))
        return send(R2, rsem.at[k, 4 + h], i, where, where, 1 - h)

    def m_g1(k, i, h, s, n):
        where = region(k, s if n == 0 else 1 - s, h, on(h))
        return send(G10 + n, rsem.at[k, h] if n == 0 else end_sem, i, where, where, h)

    def m_r1(k, i, h, s):
        where = region(k, s, h, mod(on(h) + SIDE - 1 + 2 * s))
        return send(R1, end_sem, i, where, where, h)

    def bf(v):
        return v.astype(jnp.bfloat16)

    def f32(v):
        return v.astype(jnp.float32)

    def stage_hidden(k):
        nn = ff // wd_parts
        full = max((chunks[k] - 128) // 256, 0)
        last = chunks[k] - 256 * full
        load_dy(k).wait()
        wait_gu(k)
        if k == 0:
            start_weights()
        if k == 0 and full:
            for n in range(wd_parts):
                load_wd(n).wait()

        def tile(m, size):
            rows = pl.ds(pl.multiple_of(starts[k] + m * 256, 128), size)
            part = pl.ds(pl.multiple_of(slots[k % 2] + m * 256, 128), size)
            for n in range(wd_parts):
                cols = pl.ds(n * nn, nn)
                if k == 0 and not full:
                    load_wd(n).wait()
                dh = dot(dyb[rows, :], wd[cols, :], NT)
                g, v = f32(gub[0, part, cols]), f32(gub[1, part, cols])
                sg = 1.0 / (1.0 + jnp.exp(-g))
                silu = g * sg
                dgu[rows, cols] = bf(dh * v * (sg + silu * (1.0 - sg)))
                dgu[rows, pl.ds(ff + n * nn, nn)] = bf(dh * silu)
                hid_t[cols, rows] = bf(silu * v).T

        if full:
            loop(full, lambda m: tile(m, 256))
        tile(full, last)
        if k == 0:
            start_rest()
        if k + 2 < nk:
            for c in load_gu(k + 2):
                c.start()

    def stage_a(k):
        def half(h):
            if k == 0:
                wait_w(h, 2)
            both = bf(block(k, h, mod(on(h) + 2)))
            for s in range(2):
                st_a[2 * h + s, u1(k), :] = both[s * ru(k) : (s + 1) * ru(k)]
            if k == 0:
                pl.when(h == 0)(lambda: pl.semaphore_wait(barrier, 4))
            for s in range(2):
                m_a(k, 2 * h + s, h).start()

        loop(2, half)

    def stage_b(k):
        def each(h):
            for s in range(2):
                if k == 0:
                    wait_w(h, 1 + 2 * s)
                st_b[2 * h + s, u1(k), :] = bf(term(k, 1 - s, h, mod(on(h) + 1 + 2 * s)))
            for s in range(2):
                m_b(k, 2 * h + s, h).start()

        loop(2, each)

    def stage_ct(k):
        def each(h):
            for s in range(2):
                c_term[2 * h + s, u1(k), :] = term(k, s, h, mod(on(h) + 1 + 2 * s))

        loop(2, each)

    def stage_c(k):
        def each(h):
            all_of(rsem.at[k, h], r_a.at[pl.ds(2 * h, 2), u1(k)])
            for s in range(2):
                i = 2 * h + s
                r_a[i, u1(k), :] = bf(c_term[i, u1(k), :] + f32(r_a[i, u1(k), :]))
                m_c(k, i, h).start()

        loop(2, each)

    def stage_own(k):
        def each(h):
            if k == 0:
                wait_w(h, 0)
            both = block(k, h, on(h))
            for u in range(2):
                own[h, u, u1(k), :] = both[u * ru(k) : (u + 1) * ru(k)]

        loop(2, each)

    def stage_o(k):
        def each(h):
            all_of(rsem.at[k, 2 + h], r_bc.at[h, :, u1(k)])
            for u in range(2):
                own[h, u, u1(k), :] += f32(r_bc[h, 2 + u, u1(k), :]) + f32(r_bc[h, 1 - u, u1(k), :])
            q = on(1 - h)
            for s in range(2):
                s2_ab[2 * h + s, 0, u2(k), :] = bf(own[h, s, sub(k, mod(q + 2)), :])
                s2_ab[2 * h + s, 1, u2(k), :] = bf(own[h, 1 - s, sub(k, mod(q + 1 + 2 * s)), :])
            for s in range(2):
                m_ab2(k, 2 * h + s, h).start()

        loop(2, each)

    def stage_c2(k):
        def each(h):
            all_of(rsem.at[k, 4 + h], r2_ab.at[pl.ds(2 * h, 2), :, u2(k)])
            for s in range(2):
                i = 2 * h + s
                r2_ab[i, 0, u2(k), :] = bf(own[h, s, sub(k, mod(on(1 - h) + 1 + 2 * s)), :] + f32(r2_ab[i, 0, u2(k), :]))
                m_c2(k, i, h).start()

        loop(2, each)

    def stage_o2(k):
        def each(h):
            all_of(rsem.at[k, 6 + h], r2_c.at[pl.ds(2 * h, 2), u2(k)])
            q = on(1 - h)
            for u in range(2):
                total = own[h, u, sub(k, q), :] + f32(r2_c[2 * h + u, u2(k), :]) + f32(r2_ab[2 * h + 1 - u, 1, u2(k), :])
                region(k, u, h, on(h), q)[...] = bf(total)
            for n in range(2):
                for s in range(2):
                    m_g2(k, 2 * h + s, h, s, n).start()

        loop(2, each)

    def stage_r2(k):
        def each(h):
            all_of(rsem.at[k, 2 + h], r2_c.at[pl.ds(2 * h, 2), u2(k)])
            for s in range(2):
                m_r2(k, 2 * h + s, h, s).start()

        loop(2, each)

    def stage_g1(k):
        def each(h):
            all_of(rsem.at[k, 4 + h], r2_ab.at[pl.ds(2 * h, 2), :, u2(k)])
            for n in range(2):
                for s in range(2):
                    m_g1(k, 2 * h + s, h, s, n).start()

        loop(2, each)

    def stage_r1(k):
        def each(h):
            all_of(rsem.at[k, h], r_a.at[pl.ds(2 * h, 2), u1(k)])
            for s in range(2):
                m_r1(k, 2 * h + s, h, s).start()

        loop(2, each)

    def finish():
        all_of(end_sem, r_bc)
        for kinds, ref in (((A, B, C, G10, G11, R1), st_a), ((C2, G20, G21, R2), r2_c), ((AB2,), s2_ab)):
            for kind in kinds:
                send(kind, end_sem, 0, ref, ref, 0).wait_send()

    tiles = d // nb

    def tile_gu(j):
        slot = lax.rem(j, 2)
        load_x(j, slot).wait()
        xt[...] = xb[slot].T
        pl.when(j + 2 < tiles)(lambda: load_x(j + 2, slot).start())
        nn = min(256, ff)
        rows = pl.ds(pl.multiple_of(j * nb, nb), nb)

        def cols_of(n):
            cols = pl.ds(pl.multiple_of(n * nn, nn), nn)
            dw_gate[rows, cols] = bf(dot(xt[...], dgu[:, cols], NN))
            up_cols = pl.ds(pl.multiple_of(ff + n * nn, nn), nn)
            dw_up[rows, cols] = bf(dot(xt[...], dgu[:, up_cols], NN))

        loop(ff // nn, cols_of)

    def tile_d(j):
        cols = pl.ds(pl.multiple_of(j * nb, nb), nb)
        mm = min(256, ff)

        def rows_of(m):
            rows = pl.ds(pl.multiple_of(m * mm, mm), mm)
            dw_down[rows, cols] = bf(dot(hid_t[rows, :], dyb[:, cols], NN))

        loop(ff // mm, rows_of)

    done = [0]

    def weights(n):
        lo, hi = done[0], min(done[0] + n, 2 * tiles)
        done[0] = hi
        a, b = min(lo, tiles), min(hi, tiles)
        if b > a:
            lax.fori_loop(a, b, lambda j, c: (tile_gu(j), c)[1], 0)
        a, b = max(lo, tiles) - tiles, max(hi, tiles) - tiles
        if b > a:
            lax.fori_loop(a, b, lambda j, c: (tile_d(j), c)[1], 0)

    for name, k in order():
        if name == "w":
            weights(k)
        else:
            {"h": stage_hidden, "a": stage_a, "b": stage_b, "ct": stage_ct, "c": stage_c, "own": stage_own, "o": stage_o, "c2": stage_c2,
             "o2": stage_o2, "r2": stage_r2, "g1": stage_g1, "r1": stage_r1}[name](k)
    weights(2 * tiles)
    finish()


ORDER = (
    "h0 a0 b0 h1", "a1 b1 ct0 c0", "h2 a2 h3 own0", "o0 a3 b3 ct2", "ct1 c20 w1 w1", "c1 ct3 own1 own2", "c2 o20 w1 o1",
    "b2 r20 own3 c21", "c3 o2 o21 g10", "w1 w1 w1 c22", "o3 w1 r21 r10", "w1 o22 w1 c23", "g11 w1 r22 w1", "o23 r11 r23 g12",
    "w1 w1 g13 w1", "w1 w1 r12 r13",
)


def order():
    return [(word[:-1], int(word[-1])) for words in ORDER for word in words.split()]


def write_out(*refs):
    n = (len(refs) - 1) // 2
    sem = refs[-1]
    copies = []
    for a, o in zip(refs[:n], refs[n : 2 * n]):
        parts = 2 if a.shape[0] * a.shape[1] > 2**21 else 1
        size = a.shape[0] // parts
        for i in range(parts):
            rows = pl.ds(i * size, size)
            copies.append(pltpu.make_async_copy(a.at[rows], o.at[rows], sem.at[len(copies)]))
    for c in copies:
        c.start()
    for c in copies:
        c.wait()


def solution(mesh):
    assert mesh.shape["tp"] == SIDE * SIDE

    def step(x, dy, gate, up, w_gate, w_up, w_down):
        rows, d = x.shape
        ff = gate.shape[1]
        nb = d // (2 * SIDE)
        chunks = chunk_rows(rows)
        nk = len(chunks)
        bf16, f32 = jnp.bfloat16, jnp.float32
        any_space = pl.BlockSpec(memory_space=pl.ANY)
        vmem = pl.BlockSpec(memory_space=pltpu.VMEM)
        shapes = [(rows, d), (d, ff), (d, ff), (ff, d)]
        flops = 2 * 6 * rows * d * ff
        results = pl.pallas_call(
            functools.partial(body, chunks),
            out_shape=[pltpu.VMEM(s, bf16) for s in shapes],
            in_specs=[any_space] * 7,
            out_specs=[vmem] * 4,
            scratch_shapes=[
                pltpu.VMEM((ff, d), bf16),
                pltpu.VMEM((d, 2 * ff), bf16),
                pltpu.VMEM((rows, 2 * ff), bf16),
                pltpu.VMEM((ff, rows), bf16),
                pltpu.VMEM((rows, d), bf16),
                pltpu.VMEM((2, max(chunks[::2]) + max(chunks[1::2]), ff), bf16),
                pltpu.VMEM((2, rows, nb), bf16),
                pltpu.VMEM((nb, rows), bf16),
                *[pltpu.VMEM((4, rows // 2, nb), bf16) for _ in range(3)],
                pltpu.VMEM((2, 4, rows // 2, nb), bf16),
                pltpu.VMEM((4, rows // 2, nb), f32),
                pltpu.VMEM((2, 2, rows // 2, nb), f32),
                *[pltpu.VMEM((4, 2, rows // (2 * SIDE), nb), bf16) for _ in range(2)],
                pltpu.VMEM((4, rows // (2 * SIDE), nb), bf16),
                pltpu.SemaphoreType.DMA((3 + nk + 2 * SIDE,)),
                pltpu.SemaphoreType.DMA((11,)),
                pltpu.SemaphoreType.DMA((nk, 8)),
                pltpu.SemaphoreType.DMA,
            ],
            compiler_params=pltpu.CompilerParams(
                collective_id=0, has_side_effects=True, vmem_limit_bytes=50944 * 2**10
            ),
            cost_estimate=pl.CostEstimate(flops=flops, bytes_accessed=30 * 2**20, transcendentals=rows * ff),
            name="backward",
        )(x, dy, gate, up, w_gate, w_up, w_down)
        return pl.pallas_call(
            write_out,
            out_shape=[jax.ShapeDtypeStruct(s, bf16) for s in shapes],
            in_specs=[any_space] * 4,
            out_specs=[pl.BlockSpec(memory_space=pltpu.HBM)] * 4,
            scratch_shapes=[pltpu.SemaphoreType.DMA((5,))],
            compiler_params=pltpu.CompilerParams(vmem_limit_bytes=2**20),
            name="write_out",
        )(*results)

    tokens, columns, rows = P("dp", None), P(None, "tp"), P("tp", None)
    return jax.shard_map(
        step,
        mesh=mesh,
        in_specs=(tokens, tokens, P("dp", "tp"), P("dp", "tp"), columns, columns, rows),
        out_specs=(tokens, P("dp", "tp"), P("dp", "tp"), P(("dp", "tp"), None)),
        check_vma=False,
    )
```
